256 devices in a mesh: fsdp: 64 (over z, y_lo, x), rep: 4 (over y_hi, core).
Axes of the slice: x: 4, y: 4 (y_hi: 2, y_lo: 2; y = y_hi * 2 + y_lo), z: 8, core: 2. Of those that a mesh axis runs over, the one named last changes fastest.
Arguments:
- cross_base: bfloat16 [32768, 4096], P(('fsdp', 'rep')), may hold values from -6 to 6
- layer_in: bfloat16 [32768, 4096], P(('fsdp', 'rep')), may hold values from -6 to 6
- grad_out: bfloat16 [32768, 4096], P(('fsdp', 'rep')), may hold values from -24 to 24
- reduce_a: bfloat16 [4096, 256], P('fsdp'), may hold values from -0.09375 to 0.09375
- expand_a: bfloat16 [4096, 256], P('fsdp'), may hold values from -0.375 to 0.375
- reduce_b: bfloat16 [4096, 256], P('fsdp'), may hold values from -0.09375 to 0.09375
- expand_b: bfloat16 [4096, 256], P('fsdp'), may hold values from -0.375 to 0.375
Outputs:
- grad_layer_in: bfloat16 [32768, 4096], P(('fsdp', 'rep'))
- grad_base: bfloat16 [32768, 4096], P(('fsdp', 'rep'))
- grad_reduce_a: float32 [4096, 256], P('fsdp')
- grad_expand_a: float32 [4096, 256], P('fsdp')
- grad_reduce_b: float32 [4096, 256], P('fsdp')
- grad_expand_b: float32 [4096, 256], P('fsdp')
The draws below stay inside these ranges and needn't reach their ends.
All inputs are finite; a program needn't handle non-finite values.
Results may differ from the reference program's by a relative error of at most 0.015.
Values may be sent and summed in bfloat16 or wider, within the bound.
A program may use at most 128 MiB of HBM per device.

```python
import math
import jax
import jax.numpy as jnp
from jax import lax

D = 4096
RANK = 256
TOKENS = 32768


def with_spikes(array, own_key, source, target, parts, factor):
    owner, partner = [(jnp.arange(array.shape[position]) // (array.shape[position] // parts)).reshape([-1 if axis == position else 1 for axis in range(array.ndim)]) for position in (source, target)]
    chosen = jax.random.permutation(own_key, parts)[partner]
    strong = (owner == chosen) | (owner == (partner + parts // 2) % parts)
    return jnp.where(strong, factor * array, array)


def block_scale(key, extent, split, smallest, largest):
    factor_of, own = 1.0, jax.random.fold_in(key, 6)
    for dim, parts in split:
        heights = jnp.exp(jax.random.uniform(jax.random.fold_in(own, dim), (parts,), jnp.float32, smallest / len(split), largest / len(split)))
        factor_of = factor_of * jnp.repeat(heights, extent[dim] // parts).reshape([-1 if axis == dim else 1 for axis in range(len(extent))])
    return factor_of


def gaussian(stream_key, dims, scale, most, pieces=(), kind=jnp.bfloat16):
    level = block_scale(stream_key, dims, pieces, -0.22, 0.18) if pieces else 1.0
    drawn = jax.random.normal(stream_key, dims, jnp.float32) * scale * level
    return jnp.minimum(jnp.maximum(drawn, -most), most).astype(kind)


def gaussian_with(own_key, shape, width, reach, pieces, heavy, held_as=jnp.bfloat16):
    result = width * jax.random.normal(own_key, shape, jnp.float32)
    if pieces:
        result = result * block_scale(own_key, shape, pieces, -0.22, 0.18)
    return jnp.clip(with_spikes(result, jax.random.fold_in(own_key, 3), *heavy), -reach, reach).astype(held_as)


def setup_inputs(seed: int = 0) -> dict:
    splits = jax.random.split(jax.random.key(seed), 8)
    return {
        "cross_base": gaussian(splits[0], (TOKENS, D), 1.0, 6.0, ((0, 256),)),
        "layer_in": gaussian(splits[1], (TOKENS, D), 1.0, 6.0, ((0, 256),)),
        "grad_out": gaussian_with(splits[2], (TOKENS, D), 1.0, 24.0, ((0, 256),), (0, 1, 256, 6.0)),
        "reduce_a": gaussian(splits[3], (D, RANK), D ** -0.5, 0.09375, ((0, 64),)),
        "expand_a": gaussian(splits[4], (D, RANK), RANK ** -0.5, 0.375, ((0, 64),)),
        "reduce_b": gaussian(splits[5], (D, RANK), D ** -0.5, 0.09375, ((0, 64),)),
        "expand_b": gaussian(splits[6], (D, RANK), RANK ** -0.5, 0.375, ((0, 64),)),
    }


def contract_rows(left, right):
    return lax.dot_general(left, right, (((0,), (0,)), ((), ())), preferred_element_type=jnp.float32)

def contract_cols(left, right):
    return lax.dot_general(left, right, (((1,), (1,)), ((), ())), preferred_element_type=jnp.float32)

def project(inputs, reduce_full, expand_full):
    narrow = jnp.dot(inputs, reduce_full, preferred_element_type=jnp.float32).astype(jnp.bfloat16)
    return (narrow, contract_cols(narrow, expand_full))

def local_backward(grad_in, cross_base, reduce_full, expand_full):
    grad_wide = grad_in.astype(jnp.float32)
    masked = (grad_wide * cross_base.astype(jnp.float32)).astype(jnp.bfloat16)
    narrow_grad = jnp.dot(masked, expand_full, preferred_element_type=jnp.float32).astype(jnp.bfloat16)
    passed = grad_wide + contract_cols(narrow_grad, reduce_full)
    return (masked, narrow_grad, passed)

def reference(cross_base, layer_in, grad_out, reduce_a, expand_a, reduce_b, expand_b):
    factor = 1.0 / math.sqrt(TOKENS)
    base_wide = cross_base.astype(jnp.float32)
    narrow_a, cross_a = project(layer_in, reduce_a, expand_a)
    middle = (layer_in.astype(jnp.float32) + base_wide * cross_a).astype(jnp.bfloat16)
    narrow_b, cross_b = project(middle, reduce_b, expand_b)
    masked_b, narrow_grad_b, passed_b = local_backward(grad_out, cross_base, reduce_b, expand_b)
    grad_expand_b = contract_rows(masked_b, narrow_b) * factor
    grad_reduce_b = contract_rows(middle, narrow_grad_b) * factor
    grad_middle = passed_b.astype(jnp.bfloat16)
    masked_a, narrow_grad_a, passed_a = local_backward(grad_middle, cross_base, reduce_a, expand_a)
    grad_expand_a = contract_rows(masked_a, narrow_a) * factor
    grad_reduce_a = contract_rows(layer_in, narrow_grad_a) * factor
    grad_layer_in = passed_a.astype(jnp.bfloat16)
    grad_base = (grad_out.astype(jnp.float32) * cross_b + grad_middle.astype(jnp.float32) * cross_a).astype(jnp.bfloat16)
    return (grad_layer_in, grad_base, grad_reduce_a, grad_expand_a, grad_reduce_b, grad_expand_b)
```

```python
import functools
import math

import jax
import jax.numpy as jnp
from jax import lax
from jax.experimental import pallas as pl
from jax.experimental.pallas import tpu as pltpu
from jax.sharding import PartitionSpec as P

NX, NY, NZ = 4, 4, 8
ROWS, RANK, PLANE, D, TOK = 64, 256, 512, 4096, 128
HALF = ROWS // 2
BF, F32 = jnp.bfloat16, jnp.float32
FAR = (4, 3, -3, 2, -2, 1, -1, 0)
NEAR = (0, 1, -1, 2, -2, 3, -3, 4)
UP = (0, -1, -2, -3)
R1, R2 = pl.ds(0, HALF), pl.ds(HALF, HALF)
OUTS = 4


class Place:
    def __init__(self):
        f, r = lax.axis_index("fsdp"), lax.axis_index("rep")
        self.z, self.yl, self.x = f // 8, (f // 4) % 2, f % 4
        self.yh, self.c = r // 2, r % 2
        self.y = self.yh * 2 + self.yl
        self.s = 1 - 2 * self.c
        self.oyl = 1 - self.yl
        self.planes = {d: (self.z + self.s * d + NZ) % NZ for d in range(-4, 5)}
        self.cols = {d: (self.x + self.s * d + NX) % NX for d in range(-2, 3)}

    def at(self, x, y, z, c):
        return {"fsdp": (z * 2 + y % 2) * 4 + x, "rep": (y // 2) * 2 + c}

    def dx(self, d):
        return self.at(self.cols[d], self.y, self.z, self.c)

    def dy(self, d):
        return self.at(self.x, (self.y + self.s * d + NY) % NY, self.z, self.c)

    def dz(self, d):
        return self.at(self.x, self.y, self.planes[d], self.c)

    def mate(self):
        return self.at(self.x, self.y, self.z, 1 - self.c)

    def peers(self):
        return (
            [self.dx(d) for d in (1, -1, 2)]
            + [self.dy(d) for d in (1, -1, 2)]
            + [self.dz(d) for d in (1, -1, 2, -2, 3, -3, 4)]
            + [self.mate()]
        )


class Mail:
    def __init__(self, send, recv):
        self.send, self.recv, self.ids, self.live = send, recv, {}, []

    def index(self, key):
        return self.ids.setdefault(key, len(self.ids))

    def put(self, key, src, dst, dev):
        i = self.index(key)
        copy = pltpu.make_async_remote_copy(
            src_ref=src, dst_ref=dst, send_sem=self.send.at[i], recv_sem=self.recv.at[i],
            device_id=dev, device_id_type=pl.DeviceIdType.MESH,
        )
        copy.start()
        self.live.append((key, copy))

    def got(self, key):
        for k, copy in self.live:
            if k == key:
                copy.wait_recv()
                return
        raise KeyError(key)

    def drain(self):
        for _, copy in self.live:
            copy.wait_send()


def gather_events(me, mail, w, p):
    m = 2 * p + me.c
    pn, cn, z, yl, oyl, x = me.planes, me.cols, me.z, me.yl, me.oyl, me.x
    ev = []

    def same(key, ref, dev):
        mail.put((p, 0) + key, ref, ref, dev)

    def got(*key):
        mail.got((p, 0) + key)

    def up(d):
        return 1 if d in UP else -1

    def send_1y(d):
        same(("1y", d), w.at[m, pn[d], yl, :, R1, :], me.dy(up(d)))

    def send_2y(d):
        same(("2y", d), w.at[m, pn[d], yl, x, R2, :], me.dy(up(d)))

    def send_2xa(d):
        for e in (1, -1):
            same(("2xa", d, e), w.at[m, pn[d], :, x, R2, :], me.dx(e))

    def first():
        own1, own2 = w.at[m, z, yl, x, R1, :], w.at[m, z, yl, x, R2, :]
        for d in (2, 1, -1):
            same(("1x", d), own1, me.dx(d))
        send_2y(0)
        for d in (1, -1, 2, -2, 3, -3, 4):
            same(("2z", d), own2, me.dz(d))

    def rows():
        for d in (1, -1, 2):
            got("1x", d)
        for e in (1, -1):
            same(("1z", e, 1), w.at[m, z, yl, :, R1, :], me.dz(e))
        send_1y(0)

    def zs(k):
        for d in ((k, -k) if k < 4 else (4,)):
            got("2z", -d if k < 4 else 4)
            send_2y(d)

    def xa(d):
        got("2y", d)
        send_2xa(d)

    def xb(d):
        for e in (1, -1):
            got("2xa", d, e)
        e = up(d)
        same(("2xb", d), w.at[m, pn[d], :, cn[-e], R2, :], me.dx(e))

    def hop(k):
        for e in (1, -1):
            if (e, k) == (-1, 4):
                continue
            got("1z", e, k)
            d = -e * k
            if k < 3 or (e, k) == (1, 3):
                same(("1z", e, k + 1), w.at[m, pn[d], yl, :, R1, :], me.dz(e))
            send_1y(4 if k == 4 else d)

    def d1(d):
        got("1y", d)
        same(("d1", d), w.at[m, pn[d], :, :, R1, :], me.mate())

    def d2(d):
        got("2xb", d)
        same(("d2", d), w.at[m, pn[d], :, :, R2, :], me.mate())

    def last():
        for d in NEAR:
            got("d1", d)
            got("d2", d)

    ev.append((0.0, first))
    ev.append((3.0, rows))
    ev.append((3.2, functools.partial(zs, 1)))
    ev.append((3.5, functools.partial(xa, 0)))
    ev.append((3.9, functools.partial(zs, 2)))
    ev.append((4.5, functools.partial(zs, 3)))
    ev.append((5.0, functools.partial(zs, 4)))
    for k in range(1, 5):
        t = 4.9 + 0.9 * k
        for d in ((k, -k) if k < 4 else (4,)):
            ev.append((t, functools.partial(xa, d)))
    for k in range(0, 5):
        t = 6.2 + 1.3 * k
        for d in ((k, -k) if 0 < k < 4 else (k,)):
            ev.append((t, functools.partial(xb, d)))
            ev.append((t + 2.6, functools.partial(d2, d)))
    for k in range(1, 5):
        ev.append((3.0 + 3.0 * k, functools.partial(hop, k)))
    for k in range(0, 5):
        t = 6.0 + 3.0 * k
        for d in ((k, -k) if 0 < k < 4 else (k,)):
            ev.append((t, functools.partial(d1, d)))
    ev.append((20.0, last))
    return ev


def scatter_events(me, mail, g, s, dd, st, p, scale):
    m, mo = 2 * p + me.c, 2 * p + 1 - me.c
    pn, cn, z, yl, oyl, x = me.planes, me.cols, me.z, me.yl, me.oyl, me.x
    ev = []
    up_set = (0, 1, 2, 3)

    def up(d):
        return 1 if d in up_set else -1

    def put(key, src, dst, dev):
        mail.put((p, 1) + key, src, dst, dev)

    def got(*key):
        mail.got((p, 1) + key)

    def add(where, *parts):
        tot = s[where]
        for part in parts:
            tot = tot + part
        s[where] = tot

    slot = {d: i for i, d in enumerate(FAR)}

    def swap(d):
        put(("dd", d), g.at[mo, pn[-d]], dd.at[p, pn[-d]], me.mate())

    def send_2xa(d, e):
        put(("2xa", d, e), s.at[p, pn[d], :, cn[e], R2, :], st["xa"].at[p, slot[d], (1 - e) // 2], me.dx(e))

    def join(d):
        got("dd", d)
        s[p, pn[d]] = g[m, pn[d]] + dd[p, pn[d]]
        put(("1y", d), s.at[p, pn[d], oyl, :, R1, :], st["y1"].at[p, slot[d]], me.dy(up(d)))
        put(("2xb", d), s.at[p, pn[d], :, cn[2], R2, :], st["xb"].at[p, slot[d]], me.dx(up(d)))
        send_2xa(d, -up(d))

    def xb(d):
        got("2xb", d)
        e = up(d)
        s[p, pn[d], :, cn[e], R2, :] += st["xb"][p, slot[d]]
        send_2xa(d, e)

    def xa(d):
        for e in (1, -1):
            got("2xa", d, e)
        s[p, pn[d], :, x, R2, :] += st["xa"][p, slot[d], 0] + st["xa"][p, slot[d], 1]
        put(("2y", d), s.at[p, pn[d], oyl, x, R2, :], st["y2"].at[p, slot[d]], me.dy(up(d)))

    def y2(d):
        got("2y", d)
        s[p, pn[d], yl, x, R2, :] += st["y2"][p, slot[d]]
        if d != 0:
            put(("2z", d), s.at[p, pn[d], yl, x, R2, :], st["z2"].at[p, slot[d]], me.dz(d))

    def y1(d):
        got("1y", d)
        s[p, pn[d], yl, :, R1, :] += st["y1"][p, slot[d]]

    def send_1z(e, k):
        put(("1z", e, k), s.at[p, pn[e * k], yl, :, R1, :], st["z1"].at[p, (k - 1) if e == 1 else 3 + k], me.dz(e))

    def hop(k):
        for e in (1, -1):
            if (e, k) == (-1, 4):
                continue
            got("1z", e, k)
            d = e * (k - 1)
            s[p, pn[d], yl, :, R1, :] += st["z1"][p, (k - 1) if e == 1 else 3 + k]
            if k > 1:
                send_1z(e, k - 1)

    def x1():
        for i, d in enumerate((2, 1, -1)):
            put(("1x", d), s.at[p, z, yl, cn[d], R1, :], st["x1"].at[p, i], me.dx(d))

    def done1():
        for d in (2, 1, -1):
            got("1x", d)
        tot = s[p, z, yl, x, R1, :].astype(F32)
        for i in range(3):
            tot = tot + st["x1"][p, i].astype(F32)
        st["fin"][p, 0, R1, :] = tot.astype(BF)

    def done2():
        for d in FAR[:-1]:
            got("2z", d)
        tot = s[p, z, yl, x, R2, :].astype(F32)
        for i in range(7):
            tot = tot + st["z2"][p, i].astype(F32)
        st["fin"][p, 0, R2, :] = tot.astype(BF)

    def across():
        put(("fy",), st["fin"].at[p, 0], st["fin"].at[p, 1], me.dy(2))

    def share():
        got("fy")
        st["own"][m] = (st["fin"][p, 0].astype(F32) + st["fin"][p, 1].astype(F32)) * scale
        put(("fd",), st["own"].at[m], st["own"].at[m], me.mate())

    def last():
        got("fd")

    part = functools.partial
    for d in FAR:
        ev.append((0.0, part(swap, d)))
    for i, d in enumerate(FAR):
        t = 1.5 + 0.4 * i
        ev.append((t, part(join, d)))
        ev.append((t + 3.0, part(xb, d)))
        ev.append((t + 6.0, part(xa, d)))
        ev.append((t + 9.0, part(y2, d)))
        ev.append((t + 3.2, part(y1, d)))
        if d == 4:
            ev.append((t + 3.3, part(send_1z, 1, 4)))
        if d == -3:
            ev.append((t + 3.3, part(send_1z, -1, 3)))
    for k in range(4, 0, -1):
        ev.append((8.0 + 3.0 * (4 - k), part(hop, k)))
    ev.append((17.1, x1))
    ev.append((18.0, done2))
    ev.append((20.0, done1))
    ev.append((20.1, across))
    ev.append((23.0, share))
    ev.append((25.0, last))
    return ev


def order(*lists):
    todo = [(t, n, i, f) for n, evs in enumerate(lists) for i, (t, f) in enumerate(evs)]
    for _, _, _, f in sorted(todo, key=lambda e: e[:3]):
        f()


def later(evs, dt):
    return [(t + dt, f) for t, f in evs]


def dot(a, b, dims):
    return lax.dot_general(a, b, (dims, ((), ())), preferred_element_type=F32)


NN, NT, TN = ((1,), (0,)), ((1,), (1,)), ((0,), (0,))


def kernel(
    x0_h, lin_h, go_h, ra_h, ea_h, rb_h, eb_h,
    gl_h, gb_h, o0, o1, o2, o3,
    w, g, s, dd, xa, xb, y1, y2, z1, z2, x1, fin, own,
    x0, lin, go, mid, gm, ma, mb, ca, gl, gb,
    n16, acc, send, recv, loc,
):
    me = Place()
    mail = Mail(send, recv)
    scale = 1.0 / math.sqrt(256 * TOK)
    st = dict(xa=xa, xb=xb, y1=y1, y2=y2, z1=z1, z2=z2, x1=x1, fin=fin, own=own)

    def local(i, src, dst):
        return pltpu.make_async_copy(src, dst, loc.at[i])

    loads = [local(2, lin_h, lin), local(3, x0_h, x0), local(4, go_h, go)]
    pairs = ((ra_h, ea_h), (eb_h, rb_h))

    def own_copies(c):
        return [local(p, pairs[c][p], w.at[2 * p + c, me.z, me.yl, me.x]) for p in (0, 1)]

    for c in (0, 1):
        @pl.when(me.c == c)
        def _():
            for cp in own_copies(c):
                cp.start()
    for cp in loads:
        cp.start()
    barrier = pltpu.get_barrier_semaphore()
    peers = me.peers()
    for dev in peers:
        pl.semaphore_signal(barrier, inc=1, device_id=dev, device_id_type=pl.DeviceIdType.MESH)
    pl.semaphore_wait(barrier, len(peers))
    for c in (0, 1):
        @pl.when(me.c == c)
        def _():
            for cp in own_copies(c):
                cp.wait()
    for cp in loads:
        cp.wait()

    order(gather_events(me, mail, w, 0), later(gather_events(me, mail, w, 1), 2.0))

    def plane_of(m, i):
        return w[m, i].reshape(PLANE, RANK)

    def columns(i):
        return pl.ds(pl.multiple_of(i * PLANE, PLANE), PLANE)

    def as_plane(v):
        return v.astype(BF).reshape(2, NX, ROWS, RANK)

    acc[...] = jnp.zeros_like(acc)

    @pl.loop(0, NZ)
    def _(i):
        c = columns(i)
        masked = (go[:, c].astype(F32) * x0[:, c].astype(F32)).astype(BF)
        mb[:, c] = masked
        acc[0] += dot(lin[:, c], plane_of(0, i), NN)
        acc[1] += dot(masked, plane_of(1, i), NN)

    n16[0] = acc[0].astype(BF)
    n16[1] = acc[1].astype(BF)
    acc[...] = jnp.zeros_like(acc)

    @pl.loop(0, NZ)
    def _(i):
        c = columns(i)
        base = x0[:, c].astype(F32)
        cross = dot(n16[0], plane_of(2, i), NT)
        middle = (lin[:, c].astype(F32) + base * cross).astype(BF)
        mid[:, c] = middle
        gmid = (go[:, c].astype(F32) + dot(n16[1], plane_of(3, i), NT)).astype(BF)
        gm[:, c] = gmid
        ca[:, c] = cross
        masked = (gmid.astype(F32) * base).astype(BF)
        ma[:, c] = masked
        acc[0] += dot(middle, plane_of(3, i), NN)
        acc[1] += dot(masked, plane_of(2, i), NN)
        g[0, i] = as_plane(dot(middle, n16[1], TN))
        g[1, i] = as_plane(dot(masked, n16[0], TN))

    n16[2] = acc[0].astype(BF)
    n16[3] = acc[1].astype(BF)

    @pl.loop(0, NZ)
    def _(i):
        c = columns(i)
        g[2, i] = as_plane(dot(lin[:, c], n16[3], TN))
        g[3, i] = as_plane(dot(mb[:, c], n16[2], TN))

    def results():
        @pl.loop(0, NZ)
        def _(i):
            c = columns(i)
            gmid = gm[:, c].astype(F32)
            cross = dot(n16[2], plane_of(1, i), NT)
            gb[:, c] = (go[:, c].astype(F32) * cross + gmid * ca[:, c]).astype(BF)
            gl[:, c] = (gmid + dot(n16[3], plane_of(0, i), NT)).astype(BF)

        local(0, gl, gl_h).start()
        local(1, gb, gb_h).start()

    mail2 = mail
    order(
        scatter_events(me, mail2, g, s, dd, st, 0, scale),
        later(scatter_events(me, mail2, g, s, dd, st, 1, scale), 2.0),
        [(3.0, results)],
    )
    for m, o in enumerate((o0, o1, o2, o3)):
        o[...] = own[m]
    local(0, gl, gl_h).wait()
    local(1, gb, gb_h).wait()
    mail.drain()


def on_device(cross_base, layer_in, grad_out, reduce_a, expand_a, reduce_b, expand_b):
    anywhere = pl.BlockSpec(memory_space=pl.ANY)
    vmem = pl.BlockSpec(memory_space=pltpu.VMEM)
    V = pltpu.VMEM
    gl, gb, grb, gea, gra, geb = pl.pallas_call(
        kernel,
        out_shape=[jax.ShapeDtypeStruct((TOK, D), BF)] * 2 + [jax.ShapeDtypeStruct((ROWS, RANK), F32)] * 4,
        in_specs=[anywhere] * 7,
        out_specs=[anywhere] * 2 + [vmem] * 4,
        scratch_shapes=[
            V((4, NZ, 2, NX, ROWS, RANK), BF),
            V((4, NZ, 2, NX, ROWS, RANK), BF),
            V((2, NZ, 2, NX, ROWS, RANK), BF),
            V((2, NZ, 2, NX, ROWS, RANK), BF),
            V((2, 8, 2, 2, HALF, RANK), BF),
            V((2, 8, 2, HALF, RANK), BF),
            V((2, 8, NX, HALF, RANK), BF),
            V((2, 8, HALF, RANK), BF),
            V((2, 7, NX, HALF, RANK), BF),
            V((2, 7, HALF, RANK), BF),
            V((2, 3, HALF, RANK), BF),
            V((2, 2, ROWS, RANK), BF),
            V((4, ROWS, RANK), F32),
        ]
        + [V((TOK, D), BF)] * 7
        + [V((TOK, D), F32), V((TOK, D), BF), V((TOK, D), BF)]
        + [
            V((4, TOK, RANK), BF),
            V((2, TOK, RANK), F32),
            pltpu.SemaphoreType.DMA((288,)),
            pltpu.SemaphoreType.DMA((288,)),
            pltpu.SemaphoreType.DMA((8,)),
        ],
        name="window",
        compiler_params=pltpu.CompilerParams(
            collective_id=0, has_side_effects=True, vmem_limit_bytes=62 * 1024 * 1024
        ),
    )(cross_base, layer_in, grad_out, reduce_a, expand_a, reduce_b, expand_b)
    return (gl, gb, gra, gea, grb, geb)


def solution(mesh):
    tokens, rows = P(("fsdp", "rep"), None), P("fsdp", None)
    return jax.shard_map(
        on_device,
        mesh=mesh,
        in_specs=(tokens,) * 3 + (rows,) * 4,
        out_specs=(tokens,) * 2 + (rows,) * 4,
        check_vma=False,
    )
```

```python
import functools
import math

import jax
import jax.numpy as jnp
from jax import lax
from jax.experimental import pallas as pl
from jax.experimental.pallas import tpu as pltpu
from jax.sharding import PartitionSpec as P

NX, NY, NZ = 4, 4, 8
ROWS, RANK, PLANE, D, TOK = 64, 256, 512, 4096, 128
HALF = ROWS // 2
BF, F32 = jnp.bfloat16, jnp.float32
FAR = (4, 3, -3, 2, -2, 1, -1, 0)
NEAR = (0, 1, -1, 2, -2, 3, -3, 4)
UP = (0, -1, -2, -3)
R1, R2 = pl.ds(0, HALF), pl.ds(HALF, HALF)


class Place:
    def __init__(self):
        f, r = lax.axis_index("fsdp"), lax.axis_index("rep")
        self.z, self.yl, self.x = f // 8, (f // 4) % 2, f % 4
        self.yh, self.c = r // 2, r % 2
        self.y = self.yh * 2 + self.yl
        self.s = 1 - 2 * self.c
        self.oyl = 1 - self.yl
        self.planes = {d: (self.z + self.s * d + NZ) % NZ for d in range(-4, 5)}
        self.cols = {d: (self.x + self.s * d + NX) % NX for d in range(-2, 3)}

    def at(self, x, y, z, c):
        return {"fsdp": (z * 2 + y % 2) * 4 + x, "rep": (y // 2) * 2 + c}

    def dx(self, d):
        return self.at(self.cols[d], self.y, self.z, self.c)

    def dy(self, d):
        return self.at(self.x, (self.y + self.s * d + NY) % NY, self.z, self.c)

    def dz(self, d):
        return self.at(self.x, self.y, self.planes[d], self.c)

    def mate(self):
        return self.at(self.x, self.y, self.z, 1 - self.c)

    def across(self):
        return self.at(self.x, (self.y + 2) % NY, self.z, 1 - self.c)

    def peers(self):
        return (
            [self.dx(d) for d in (1, -1, 2)]
            + [self.dy(d) for d in (1, -1, 2)]
            + [self.dz(d) for d in (1, -1, 2, -2, 3, -3, 4)]
            + [self.mate(), self.across()]
        )


class Mail:
    def __init__(self, send, recv):
        self.send, self.recv, self.ids, self.live = send, recv, {}, []

    def index(self, key):
        return self.ids.setdefault(key, len(self.ids))

    def put(self, key, src, dst, dev):
        i = self.index(key)
        copy = pltpu.make_async_remote_copy(
            src_ref=src, dst_ref=dst, send_sem=self.send.at[i], recv_sem=self.recv.at[i],
            device_id=dev, device_id_type=pl.DeviceIdType.MESH,
        )
        copy.start()
        self.live.append((key, copy))

    def got(self, key):
        for k, copy in self.live:
            if k == key:
                copy.wait_recv()
                return
        raise KeyError(key)

    def drain(self):
        for _, copy in self.live:
            copy.wait_send()


def gather_events(me, mail, w, p, use, sequence, start, step):
    m = 2 * p + me.c
    pn, cn, z, yl, oyl, x = me.planes, me.cols, me.z, me.yl, me.oyl, me.x
    ev = []

    def same(key, ref, dev):
        mail.put((p, 0) + key, ref, ref, dev)

    def got(*key):
        mail.got((p, 0) + key)

    def up(d):
        return 1 if d in UP else -1

    def send_1y(d):
        same(("1y", d), w.at[m, pn[d], yl, :, R1, :], me.dy(up(d)))

    def send_2y(d):
        same(("2y", d), w.at[m, pn[d], yl, x, R2, :], me.dy(up(d)))

    def send_2xa(d):
        for e in (1, -1):
            same(("2xa", d, e), w.at[m, pn[d], :, x, R2, :], me.dx(e))

    def first():
        own1, own2 = w.at[m, z, yl, x, R1, :], w.at[m, z, yl, x, R2, :]
        for d in (2, 1, -1):
            same(("1x", d), own1, me.dx(d))
        send_2y(0)
        for d in (1, -1, 2, -2, 3, -3, 4):
            same(("2z", d), own2, me.dz(d))

    def rows():
        for d in (1, -1, 2):
            got("1x", d)
        for k in (1, 2):
            for e in (1, -1):
                same(("1z", e, k), w.at[m, z, yl, :, R1, :], me.dz(k * e))
        send_1y(0)

    def zs(k):
        for d in ((k, -k) if k < 4 else (4,)):
            got("2z", -d if k < 4 else 4)
            send_2y(d)

    def xa(d):
        got("2y", d)
        send_2xa(d)

    def xb(d):
        for e in (1, -1):
            got("2xa", d, e)
        e = up(d)
        same(("2xb", d), w.at[m, pn[d], :, cn[-e], R2, :], me.dx(e))

    def near():
        for e in (1, -1):
            got("1z", e, 1)
            send_1y(-e)

    def relay():
        for e in (1, -1):
            got("1z", e, 2)
            block = w.at[m, pn[-2 * e], yl, :, R1, :]
            same(("1z", e, 3), block, me.dz(e))
            if e == 1:
                same(("1z", e, 4), block, me.dz(2))
            send_1y(-2 * e)

    def far():
        for e in (1, -1):
            got("1z", e, 3)
            send_1y(-3 * e)
        got("1z", 1, 4)
        send_1y(4)

    def d1(d):
        got("1y", d)
        same(("d1", d), w.at[m, pn[d], :, :, R1, :], me.mate())

    def d2(d):
        got("2xb", d)
        same(("d2", d), w.at[m, pn[d], :, :, R2, :], me.mate())

    def ready(d):
        got("d1", -d if abs(d) < 4 else d)
        got("d2", -d if abs(d) < 4 else d)
        use(d)

    part = functools.partial
    ev.append((0.0, first))
    ev.append((3.0, rows))
    for k in range(1, 5):
        ev.append((2.6 + 0.5 * k, part(zs, k)))
    ev.append((6.1, near))
    ev.append((6.6, relay))
    ev.append((9.6, far))
    for d in NEAR:
        k = abs(d)
        ev.append((5.8 + 0.5 * k if k else 3.3, part(xa, d)))
        ev.append((8.9 + 0.5 * k if k else 6.4, part(xb, d)))
        ev.append((12.1 + 0.5 * k if k else 9.6, part(d2, d)))
        ev.append(((6.5, 9.5, 9.8, 12.7, 12.9)[k], part(d1, d)))
    for i, d in enumerate(sequence):
        ev.append((start + step * i, part(ready, d)))
    return ev


def scatter_events(me, mail, g, s, dd, st, p, scale, step):
    m, mo = 2 * p + me.c, 2 * p + 1 - me.c
    pn, cn, z, yl, oyl, x = me.planes, me.cols, me.z, me.yl, me.oyl, me.x
    ev = []
    up_set = (0, 1, 2, 3)

    def up(d):
        return 1 if d in up_set else -1

    def put(key, src, dst, dev):
        mail.put((p, 1) + key, src, dst, dev)

    def got(*key):
        mail.got((p, 1) + key)

    def add(where, *parts):
        tot = s[where]
        for part in parts:
            tot = tot + part
        s[where] = tot

    slot = {d: i for i, d in enumerate(FAR)}

    def swap(d):
        put(("dd", d), g.at[mo, pn[-d]], dd.at[p, pn[-d]], me.mate())

    def send_2xa(d, e):
        put(("2xa", d, e), s.at[p, pn[d], :, cn[e], R2, :], st["xa"].at[p, slot[d], (1 - e) // 2], me.dx(e))

    def join(d):
        got("dd", d)
        s[p, pn[d]] = g[m, pn[d]] + dd[p, pn[d]]
        put(("1y", d), s.at[p, pn[d], oyl, :, R1, :], st["y1"].at[p, slot[d]], me.dy(up(d)))
        put(("2xb", d), s.at[p, pn[d], :, cn[2], R2, :], st["xb"].at[p, slot[d]], me.dx(up(d)))
        send_2xa(d, -up(d))

    def xb(d):
        got("2xb", d)
        e = up(d)
        s[p, pn[d], :, cn[e], R2, :] += st["xb"][p, slot[d]]
        send_2xa(d, e)

    def xa(d):
        for e in (1, -1):
            got("2xa", d, e)
        s[p, pn[d], :, x, R2, :] += st["xa"][p, slot[d], 0] + st["xa"][p, slot[d], 1]
        put(("2y", d), s.at[p, pn[d], oyl, x, R2, :], st["y2"].at[p, slot[d]], me.dy(up(d)))

    def y2(d):
        got("2y", d)
        s[p, pn[d], yl, x, R2, :] += st["y2"][p, slot[d]]
        if d != 0:
            put(("2z", d), s.at[p, pn[d], yl, x, R2, :], st["z2"].at[p, slot[d]], me.dz(d))

    def y1(d):
        got("1y", d)
        s[p, pn[d], yl, :, R1, :] += st["y1"][p, slot[d]]
        if d == 4:
            send_1z(1, 4)
        elif abs(d) in (1, 3):
            send_1z(1 if d > 0 else -1, abs(d))

    def send_1z(e, k):
        hops = {1: e, 2: 2 * e, 3: e, 4: 2}[k]
        put(("1z", e, k), s.at[p, pn[e * k], yl, :, R1, :], st["z1"].at[p, slot1(e, k)], me.dz(hops))

    def slot1(e, k):
        return k - 1 if e == 1 else 3 + k

    def add1(e, k, d):
        got("1z", e, k)
        s[p, pn[d], yl, :, R1, :] += st["z1"][p, slot1(e, k)]

    def meet():
        add1(1, 4, 2)
        for e in (1, -1):
            add1(e, 3, 2 * e)
            send_1z(e, 2)

    def home():
        for k in (1, 2):
            for e in (1, -1):
                add1(e, k, 0)
        x1()

    def x1():
        for i, d in enumerate((2, 1, -1)):
            put(("1x", d), s.at[p, z, yl, cn[d], R1, :], st["x1"].at[p, i], me.dx(d))

    def done1():
        for d in (2, 1, -1):
            got("1x", d)
        tot = s[p, z, yl, x, R1, :].astype(F32)
        for i in range(3):
            tot = tot + st["x1"][p, i].astype(F32)
        st["fin"][p, 0, R1, :] = tot.astype(BF)

    def done2():
        for d in FAR[:-1]:
            got("2z", d)
        tot = s[p, z, yl, x, R2, :].astype(F32)
        for i in range(7):
            tot = tot + st["z2"][p, i].astype(F32)
        st["fin"][p, 0, R2, :] = tot.astype(BF)

    def across():
        for i, dev in ((1, me.mate()), (2, me.dy(2)), (3, me.across())):
            put(("f", i), st["fin"].at[p, 0], st["fin"].at[p, i], dev)

    def share():
        for i in (1, 2, 3):
            got("f", i)
        half = [st["fin"][p, i].astype(F32) for i in range(4)]
        st["own"][m] = (half[0] + half[2]) * scale
        st["own"][mo] = (half[1] + half[3]) * scale

    part = functools.partial
    for i, d in enumerate(FAR):
        t = step * i
        ev.append((t, part(join, d)))
        ev.append((t + 3.0, part(xb, d)))
        ev.append((t + 6.0, part(xa, d)))
        ev.append((t + 9.0, part(y2, d)))
        ev.append((t + 3.2, part(y1, d)))
    end = step * 7
    ev.append((end + 3.4, meet))
    ev.append((end + 6.6, home))
    ev.append((end + 9.9, done1))
    ev.append((end + 12.5, done2))
    ev.append((end + 12.6, across))
    ev.append((end + 15.6, share))
    return ev, swap


def order(*lists):
    todo = [(t, n, i, f) for n, evs in enumerate(lists) for i, (t, f) in enumerate(evs)]
    for _, _, _, f in sorted(todo, key=lambda e: e[:3]):
        f()


def later(evs, dt):
    return [(t + dt, f) for t, f in evs]


def dot(a, b, dims):
    return lax.dot_general(a, b, (dims, ((), ())), preferred_element_type=F32)


NN, NT, TN = ((1,), (0,)), ((1,), (1,)), ((0,), (0,))


def kernel(
    x0_h, lin_h, go_h, ra_h, ea_h, rb_h, eb_h,
    big_h, small,
    w, g, s, dd, xa, xb, y1, y2, z1, z2, x1, fin, own,
    x0, lin, go, gm, mb, ca, big,
    n16, acc, send, recv, loc,
):
    me = Place()
    mail = Mail(send, recv)
    scale = 1.0 / math.sqrt(256 * TOK)
    st = dict(xa=xa, xb=xb, y1=y1, y2=y2, z1=z1, z2=z2, x1=x1, fin=fin, own=own)

    def local(i, src, dst):
        return pltpu.make_async_copy(src, dst, loc.at[i])

    loads = [local(2, lin_h, lin), local(3, x0_h, x0), local(4, go_h, go)]
    pairs = ((ra_h, ea_h), (eb_h, rb_h))

    def own_copies(c):
        return [local(p, pairs[c][p], w.at[2 * p + c, me.z, me.yl, me.x]) for p in (0, 1)]

    for c in (0, 1):
        @pl.when(me.c == c)
        def _():
            for cp in own_copies(c):
                cp.start()
    for cp in loads:
        cp.start()
    barrier = pltpu.get_barrier_semaphore()
    peers = me.peers()
    for dev in peers:
        pl.semaphore_signal(barrier, inc=1, device_id=dev, device_id_type=pl.DeviceIdType.MESH)
    pl.semaphore_wait(barrier, len(peers))
    for c in (0, 1):
        @pl.when(me.c == c)
        def _():
            for cp in own_copies(c):
                cp.wait()

    def plane_of(m, i):
        return w[m, i].reshape(PLANE, RANK)

    def columns(i):
        return pl.ds(pl.multiple_of(i * PLANE, PLANE), PLANE)

    def as_plane(v):
        return v.astype(BF).reshape(2, NX, ROWS, RANK)

    rs0, swap0 = scatter_events(me, mail, g, s, dd, st, 0, scale, 0.7)
    rs1, swap1 = scatter_events(me, mail, g, s, dd, st, 1, scale, 0.4)

    def loaded():
        for cp in loads:
            cp.wait()
        acc[...] = jnp.zeros_like(acc)

    def enter(d):
        i = me.planes[d]
        c = columns(i)
        masked = (go[:, c].astype(F32) * x0[:, c].astype(F32)).astype(BF)
        mb[:, c] = masked
        acc[0] += dot(lin[:, c], plane_of(0, i), NN)
        acc[1] += dot(masked, plane_of(1, i), NN)

    def narrow(a):
        n16[a] = acc[0].astype(BF)
        n16[a + 1] = acc[1].astype(BF)
        acc[...] = jnp.zeros_like(acc)

    def middle(d):
        i = me.planes[d]
        c = columns(i)
        base = x0[:, c].astype(F32)
        cross = dot(n16[0], plane_of(2, i), NT)
        mid = (lin[:, c].astype(F32) + base * cross).astype(BF)
        gmid = (go[:, c].astype(F32) + dot(n16[1], plane_of(3, i), NT)).astype(BF)
        gm[:, c] = gmid
        ca[:, c] = cross
        masked = (gmid.astype(F32) * base).astype(BF)
        g[0, i] = as_plane(dot(mid, n16[1], TN))
        g[1, i] = as_plane(dot(masked, n16[0], TN))
        swap0(-d if d != 4 else d)
        acc[0] += dot(mid, plane_of(3, i), NN)
        acc[1] += dot(masked, plane_of(2, i), NN)

    def outer(d):
        i = me.planes[d]
        c = columns(i)
        g[2, i] = as_plane(dot(lin[:, c], n16[3], TN))
        g[3, i] = as_plane(dot(mb[:, c], n16[2], TN))
        swap1(-d if d != 4 else d)

    def result(i):
        c = pl.ds(i * PLANE, PLANE)
        gmid = gm[:, c].astype(F32)
        cross = dot(n16[2], plane_of(1, i), NT)
        big[1, :, c] = (go[:, c].astype(F32) * cross + gmid * ca[:, c]).astype(BF)
        big[0, :, c] = (gmid + dot(n16[3], plane_of(0, i), NT)).astype(BF)

    def write():
        local(0, big, big_h).start()

    part = functools.partial
    order(
        gather_events(me, mail, w, 0, enter, NEAR, 13.0, 0.5),
        later(gather_events(me, mail, w, 1, middle, FAR, 15.4, 0.7), 3.0),
        [(12.9, loaded), (17.0, part(narrow, 0)), (24.1, part(narrow, 2))],
        [(24.2 + 0.4 * i, part(outer, d)) for i, d in enumerate(FAR)],
        later(rs0, 20.0),
        later(rs1, 26.0),
        [(29.5 + 1.0 * i, part(result, i)) for i in range(NZ)] + [(37.6, write)],
    )
    small[...] = own[...]
    local(0, big, big_h).wait()
    mail.drain()


def on_device(cross_base, layer_in, grad_out, reduce_a, expand_a, reduce_b, expand_b):
    anywhere = pl.BlockSpec(memory_space=pl.ANY)
    vmem = pl.BlockSpec(memory_space=pltpu.VMEM)
    V = pltpu.VMEM
    big, small = pl.pallas_call(
        kernel,
        out_shape=[jax.ShapeDtypeStruct((2, TOK, D), BF), jax.ShapeDtypeStruct((4, ROWS, RANK), F32)],
        in_specs=[anywhere] * 7,
        out_specs=[anywhere, vmem],
        scratch_shapes=[
            V((4, NZ, 2, NX, ROWS, RANK), BF),
            V((4, NZ, 2, NX, ROWS, RANK), BF),
            V((2, NZ, 2, NX, ROWS, RANK), BF),
            V((2, NZ, 2, NX, ROWS, RANK), BF),
            V((2, 8, 2, 2, HALF, RANK), BF),
            V((2, 8, 2, HALF, RANK), BF),
            V((2, 8, NX, HALF, RANK), BF),
            V((2, 8, HALF, RANK), BF),
            V((2, 7, NX, HALF, RANK), BF),
            V((2, 7, HALF, RANK), BF),
            V((2, 3, HALF, RANK), BF),
            V((2, 4, ROWS, RANK), BF),
            V((4, ROWS, RANK), F32),
        ]
        + [V((TOK, D), BF)] * 5
        + [V((TOK, D), F32), V((2, TOK, D), BF)]
        + [
            V((4, TOK, RANK), BF),
            V((2, TOK, RANK), F32),
            pltpu.SemaphoreType.DMA((288,)),
            pltpu.SemaphoreType.DMA((288,)),
            pltpu.SemaphoreType.DMA((8,)),
        ],
        name="window",
        compiler_params=pltpu.CompilerParams(
            collective_id=0, has_side_effects=True, vmem_limit_bytes=62 * 1024 * 1024
        ),
    )(cross_base, layer_in, grad_out, reduce_a, expand_a, reduce_b, expand_b)
    return (big[0], big[1], small[2], small[1], small[0], small[3])


def solution(mesh):
    tokens, rows = P(("fsdp", "rep"), None), P("fsdp", None)
    return jax.shard_map(
        on_device,
        mesh=mesh,
        in_specs=(tokens,) * 3 + (rows,) * 4,
        out_specs=(tokens,) * 2 + (rows,) * 4,
        check_vma=False,
    )
```
